32 devices in a mesh: dp: 4 (over y, x), sub: 8 (over z, core).
Axes of the slice: x: 2, y: 2, z: 4, core: 2. Of those that a mesh axis runs over, the one named last changes fastest.
Arguments:
- embeddings: bfloat16 [12288, 1024], P('dp'), may hold values from -4096 to 4096
- assignment: int32 [12288], P('dp'), may hold values from 0 to 4095
- centroids: bfloat16 [4096, 1024], P('sub'), may hold values from -1 to 1
- codebooks: float32 [64, 16, 256], P('sub'), may hold values from -2 to 2
Outputs:
- new_centroids: float32 [4096, 1024], P('sub')
- new_codebooks: float32 [64, 16, 256], P('sub')
The draws below stay inside these ranges and needn't reach their ends.
All inputs are finite; a program needn't handle non-finite values.
Results may differ from the reference program's by a relative error of at most 0.0004.
The reference program's roundings to bfloat16 on the way count: a program that leaves them out, or rounds other values in their place, can miss the bound.
Values may be sent and summed in bfloat16 or wider, within the bound.
No kernel may reach another device: no remote copies, remote signals or barrier semaphores. Data moves between devices by JAX's collectives and lax.ppermute only.
A program may use at most 128 MiB of HBM per device.

```python
import math
import jax
import jax.numpy as jnp
from jax import lax

D = 1024
K = 4096
M = 64
CW = 256
ROW_DEV = 3072
SUB_DIM = 16
ROWS = 12288
N_DP = 4


def joint_draw(key):
    key_list = jax.random.split(jax.random.fold_in(key, 4242), 5)
    assign_ids = jax.random.randint(key_list[0], (ROWS,), 0, K, dtype=jnp.int32)
    cent_scale = 0.6 / math.sqrt(D)
    cent_values = jnp.clip(jax.random.normal(key_list[1], (K, D), jnp.float32), -4.0, 4.0) * cent_scale
    code_values = jnp.clip(jax.random.normal(key_list[2], (M, SUB_DIM, CW), jnp.float32), -6.0, 6.0) * 0.3
    row_scale = jnp.exp(jnp.log(3.0) * jnp.arange(ROWS, dtype=jnp.float32) / ROWS + jax.random.uniform(key_list[3], (ROWS,), jnp.float32, 0.0, math.log(4.0)))
    sample = jnp.clip(jax.random.normal(key_list[4], (ROWS, D), jnp.float32), -4.0, 4.0)
    sample = sample * row_scale[:, None]
    sample = jnp.clip(sample, -4096.0, 4096.0)
    return (sample, assign_ids, cent_values, code_values)


def draw_embeddings(key, part):
    return joint_draw(key)[0].astype(jnp.bfloat16)


def draw_assignment(key, part):
    return joint_draw(key)[1]


def draw_centroids(key, part):
    return joint_draw(key)[2].astype(jnp.bfloat16)


def draw_codebooks(key, part):
    return joint_draw(key)[3]


def setup_inputs(seed: int = 0) -> dict:
    seeds = jax.random.split(jax.random.key(seed), 5)
    return {
        "embeddings": draw_embeddings(jax.random.fold_in(seeds[4], 71), 0),
        "assignment": draw_assignment(jax.random.fold_in(seeds[4], 71), 0),
        "centroids": draw_centroids(jax.random.fold_in(seeds[4], 71), 0),
        "codebooks": draw_codebooks(jax.random.fold_in(seeds[4], 71), 0),
    }


def reference(embeddings, assignment, centroids, codebooks):
    cent_float = centroids.astype(jnp.float32)
    half_norm = 0.5 * jnp.sum(cent_float * cent_float, axis=1)
    code_half = 0.5 * jnp.sum(codebooks * codebooks, axis=1)
    row_tiles = embeddings.reshape(N_DP, ROW_DEV, D)
    tile_ids = assignment.reshape(N_DP, ROW_DEV)

    def accumulate(running, pieces):
        tile_rows, tile_assign = pieces
        logits = jnp.dot(tile_rows, centroids.T, preferred_element_type=jnp.float32) - half_norm[None, :]
        expo_terms = jnp.exp(logits - jnp.max(logits, axis=1, keepdims=True))
        probability = expo_terms / jnp.sum(expo_terms, axis=1, keepdims=True)
        cent_sums = running[0] + jnp.dot(probability.astype(jnp.bfloat16).T, tile_rows, preferred_element_type=jnp.float32)
        cent_counts = running[1] + jnp.sum(probability, axis=0)
        base_rows = jnp.take(centroids, tile_assign.astype(jnp.int32), axis=0).astype(jnp.float32)
        res_parts = (tile_rows.astype(jnp.float32) - base_rows).reshape(ROW_DEV, M, SUB_DIM)
        code_logits = jnp.einsum("rsd,sdc->rsc", res_parts, codebooks, precision=lax.Precision.HIGHEST) - code_half[None]
        code_exp = jnp.exp(code_logits - jnp.max(code_logits, axis=2, keepdims=True))
        code_weights = code_exp / jnp.sum(code_exp, axis=2, keepdims=True)
        code_sums = running[2] + jnp.einsum("rsc,rsd->sdc", code_weights, res_parts, precision=lax.Precision.HIGHEST)
        code_counts = running[3] + jnp.sum(code_weights, axis=0)
        return (cent_sums, cent_counts, code_sums, code_counts), None

    initial = (jnp.zeros((K, D), jnp.float32), jnp.zeros((K,), jnp.float32),
               jnp.zeros((M, SUB_DIM, CW), jnp.float32), jnp.zeros((M, CW), jnp.float32))
    final_state, unused = lax.scan(accumulate, initial, (row_tiles, tile_ids))
    new_centroids = (final_state[0] + cent_float) / (final_state[1][:, None] + 1.0)
    new_codebooks = (final_state[2] + codebooks) / (final_state[3][:, None, :] + 1.0)
    return new_centroids, new_codebooks
```

```python
import functools
import math

import jax
import jax.numpy as jnp
from jax import lax
from jax.experimental import pallas as pl
from jax.experimental.pallas import tpu as pltpu
from jax.sharding import PartitionSpec as P


F32 = jnp.float32
BF16 = jnp.bfloat16
VMEM = pltpu.VMEM
SMEM = pltpu.SMEM
NT = (((1,), (1,)), ((), ()))


def swap(value, axis, size, hop):
    return lax.ppermute(value, axis, [(i, i ^ hop) for i in range(size)])


def block_of(extent, want):
    return want if extent % want == 0 else extent


def params(limit=56 << 20):
    return pltpu.CompilerParams(vmem_limit_bytes=limit)


def table_kernel(pos_ref, cent_ref, *refs, width):
    outs, flip_ref = refs[:-1], refs[-1]
    flip_ref[...] = cent_ref[...].T
    for hop, out_ref in enumerate(outs):
        start = pl.multiple_of((pos_ref[0] ^ hop) * width, width)
        out_ref[...] = flip_ref[pl.ds(start, width), :]


def table_parts(position, centroids, peers):
    local_k, feat = centroids.shape
    width = feat // peers
    return pl.pallas_call(
        functools.partial(table_kernel, width=width),
        out_shape=[jax.ShapeDtypeStruct((width, local_k), BF16)] * peers,
        in_specs=[pl.BlockSpec(memory_space=SMEM), pl.BlockSpec(memory_space=VMEM)],
        out_specs=[pl.BlockSpec(memory_space=VMEM)] * peers,
        scratch_shapes=[VMEM((feat, local_k), BF16)],
        compiler_params=params(),
        name="table_parts",
    )(position, centroids)


def logits_kernel(cent_ref, rows_ref, logits_ref, stats_ref, half_ref):
    @pl.when(pl.program_id(0) == 0)
    def _():
        wide = cent_ref[...].astype(F32)
        half_ref[...] = jnp.broadcast_to(
            0.5 * jnp.sum(wide * wide, axis=1, keepdims=True), half_ref.shape
        )

    logits = (
        lax.dot_general(cent_ref[...], rows_ref[...], NT, preferred_element_type=F32)
        - half_ref[:, 0:1]
    )
    logits_ref[...] = logits
    peak = jnp.max(logits, axis=0, keepdims=True)
    stats_ref[0:1, :] = peak
    stats_ref[1:2, :] = jnp.sum(jnp.exp(logits - peak), axis=0, keepdims=True)


def local_logits(centroids, embeddings):
    local_k, feat = centroids.shape
    rows = embeddings.shape[0]
    block = block_of(rows, 512)
    return pl.pallas_call(
        logits_kernel,
        grid=(rows // block,),
        out_shape=[
            jax.ShapeDtypeStruct((local_k, rows), F32),
            jax.ShapeDtypeStruct((2, rows), F32),
        ],
        in_specs=[
            pl.BlockSpec((local_k, feat), lambda i: (0, 0)),
            pl.BlockSpec((block, feat), lambda i: (i, 0)),
        ],
        out_specs=[
            pl.BlockSpec((local_k, block), lambda i: (0, i)),
            pl.BlockSpec((2, block), lambda i: (0, i)),
        ],
        scratch_shapes=[VMEM((local_k, 128), F32)],
        compiler_params=params(),
        cost_estimate=pl.CostEstimate(
            flops=2 * local_k * rows * feat,
            transcendentals=local_k * rows,
            bytes_accessed=rows * feat * 2 + local_k * rows * 4,
        ),
        name="local_logits",
    )(centroids, embeddings)


def merge(former, latter):
    peak = jnp.maximum(former[0:1], latter[0:1])
    total = former[1:2] * jnp.exp(former[0:1] - peak) + latter[1:2] * jnp.exp(latter[0:1] - peak)
    return jnp.concatenate([peak, total], axis=0)


def sums_kernel(pos_ref, logits_ref, stats_ref, rows_ref, *refs, peers):
    outs, counts, (acc_ref, count_ref) = refs[:peers], refs[peers : 2 * peers], refs[2 * peers :]
    step = pl.program_id(0)
    probability = jnp.exp(logits_ref[...] - stats_ref[0:1, :]) * (1.0 / stats_ref[1:2, :])
    partial = probability[:, 0:128]
    for lane in range(128, probability.shape[1], 128):
        partial = partial + probability[:, lane : lane + 128]
    sums = jnp.dot(probability.astype(BF16), rows_ref[...], preferred_element_type=F32)

    @pl.when(step == 0)
    def _():
        acc_ref[...] = sums
        count_ref[...] = partial

    @pl.when(step > 0)
    def _():
        acc_ref[...] += sums
        count_ref[...] += partial

    @pl.when(step == pl.num_programs(0) - 1)
    def _():
        part = outs[0].shape[0]
        for hop in range(peers):
            start = pl.multiple_of((pos_ref[0] ^ hop) * part, part)
            outs[hop][...] = acc_ref[pl.ds(start, part), :]
            counts[hop][...] = jnp.broadcast_to(
                jnp.sum(count_ref[pl.ds(start, part), :], axis=1, keepdims=True), counts[hop].shape
            )


def local_sums(position, logits, stats, embeddings, peers):
    local_k, rows = logits.shape
    feat = embeddings.shape[1]
    block = block_of(rows, 512)
    part = local_k // peers
    whole = lambda shape: pl.BlockSpec(shape, lambda i: (0, 0))
    return pl.pallas_call(
        functools.partial(sums_kernel, peers=peers),
        grid=(rows // block,),
        out_shape=[jax.ShapeDtypeStruct((part, feat), F32)] * peers
        + [jax.ShapeDtypeStruct((part, 128), F32)] * peers,
        in_specs=[
            pl.BlockSpec(memory_space=SMEM),
            pl.BlockSpec((local_k, block), lambda i: (0, i)),
            pl.BlockSpec((2, block), lambda i: (0, i)),
            pl.BlockSpec((block, feat), lambda i: (i, 0)),
        ],
        out_specs=[whole((part, feat))] * peers + [whole((part, 128))] * peers,
        scratch_shapes=[VMEM((local_k, feat), F32), VMEM((local_k, 128), F32)],
        compiler_params=params(),
        cost_estimate=pl.CostEstimate(
            flops=2 * local_k * rows * feat,
            transcendentals=local_k * rows,
            bytes_accessed=rows * feat * 2 + local_k * rows * 4,
        ),
        name="local_sums",
    )(position, logits, stats, embeddings)


def update_kernel(pos_ref, cent_ref, *refs, peers):
    sums, counts, out_ref = refs[:peers], refs[peers : 2 * peers], refs[2 * peers]
    part = out_ref.shape[0]
    total, count = sums[0][...], counts[0][...]
    for hop in range(1, peers):
        total = total + sums[hop][...]
        count = count + counts[hop][...]
    start = pl.multiple_of(pos_ref[0] * part, part)
    out_ref[...] = (total + cent_ref[pl.ds(start, part), :].astype(F32)) / (count[:, 0:1] + 1.0)


def update_part(position, centroids, sums, counts):
    peers = len(sums)
    return pl.pallas_call(
        functools.partial(update_kernel, peers=peers),
        out_shape=jax.ShapeDtypeStruct(sums[0].shape, F32),
        in_specs=[pl.BlockSpec(memory_space=SMEM)] + [pl.BlockSpec(memory_space=VMEM)] * (1 + 2 * peers),
        out_specs=pl.BlockSpec(memory_space=VMEM),
        compiler_params=params(),
        name="update_part",
    )(position, centroids, *sums, *counts)


def join_kernel(pos_ref, *refs):
    parts, out_ref = refs[:-1], refs[-1]
    size = parts[0].shape[0]
    for hop, part_ref in enumerate(parts):
        start = pl.multiple_of((pos_ref[0] ^ hop) * size, size)
        out_ref[pl.ds(start, size), :] = part_ref[...]


def join_parts(position, parts):
    size, feat = parts[0].shape
    return pl.pallas_call(
        join_kernel,
        out_shape=jax.ShapeDtypeStruct((size * len(parts), feat), F32),
        in_specs=[pl.BlockSpec(memory_space=SMEM)] + [pl.BlockSpec(memory_space=VMEM)] * len(parts),
        out_specs=pl.BlockSpec(memory_space=VMEM),
        compiler_params=params(),
        name="join_parts",
    )(position, *parts)


def three_terms(value):
    first = value.astype(BF16)
    rest = value - first.astype(F32)
    second = rest.astype(BF16)
    third = (rest - second.astype(F32)).astype(BF16)
    return first, second, third


def codes_kernel(pick_ref, feats_ref, code_ref, *refs, peers):
    tables, (out_ref, table_ref, weight_ref, data_ref, acc_ref) = refs[:peers], refs[peers:]
    step = pl.program_id(0)
    groups, sub_dim, words = code_ref.shape
    width, local_k = tables[0].shape
    block = feats_ref.shape[0]
    depth = data_ref.shape[1]
    head = 3 * sub_dim

    @pl.when(step == 0)
    def _():
        for hop in range(peers):
            table_ref[hop * width : (hop + 1) * width, :] = tables[hop][...]
        scale = 1.0 / math.log(2.0)
        lane_row = lax.broadcasted_iota(jnp.int32, (sub_dim, words), 0)
        for group in range(groups):
            code = code_ref[group]
            first, second, third = three_terms(code * scale)
            half = -0.5 * scale * jnp.sum(code * code, axis=0, keepdims=True)
            bias = [jnp.broadcast_to(t.astype(F32), (sub_dim, words)) for t in three_terms(half)]
            bias = jnp.where(
                lane_row == 0, bias[0], jnp.where(lane_row == 1, bias[1], jnp.where(lane_row == 2, bias[2], 0.0))
            )
            first, second, third = (t.astype(F32) for t in (first, second, third))
            stacked = jnp.concatenate([first, first, bias, second, second, third, third], axis=0)
            weight_ref[group * words : (group + 1) * words, :] = stacked.T.astype(BF16)
        acc_ref[...] = jnp.zeros_like(acc_ref)
        for group in range(groups):
            data_ref[group, 2 * sub_dim : 3 * sub_dim, :] = jnp.ones((sub_dim, block), BF16)

    source, entry = pick_ref[0:1, :], pick_ref[1:2, :]
    hot = (lax.broadcasted_iota(jnp.int32, (local_k, block), 0) == entry).astype(F32).astype(BF16)
    slabs = jnp.dot(table_ref[...], hot, preferred_element_type=F32)
    base = slabs[0:width]
    for hop in range(1, peers):
        base = jnp.where(source == hop, slabs[hop * width : (hop + 1) * width], base)
    minus = (-base).astype(BF16)
    own = feats_ref[...].astype(F32).T.astype(BF16)
    for group in range(groups):
        span = slice(group * sub_dim, (group + 1) * sub_dim)
        for at in (0, 3, 5):
            data_ref[group, at * sub_dim : (at + 1) * sub_dim, :] = own[span]
            data_ref[group, (at + 1) * sub_dim : (at + 2) * sub_dim, :] = minus[span]
    for group in range(groups):
        logits = jnp.dot(
            weight_ref[group * words : (group + 1) * words, :], data_ref[group], preferred_element_type=F32
        )
        expo = jnp.exp2(logits - jnp.max(logits, axis=0, keepdims=True))
        weights = expo * (1.0 / jnp.sum(expo, axis=0, keepdims=True))
        high = weights.astype(BF16)
        low = (weights - high.astype(F32)).astype(BF16)
        left = data_ref[group, 0:head, :]
        acc_ref[group] += lax.dot_general(high, left, NT, preferred_element_type=F32) + lax.dot_general(
            low, left, NT, preferred_element_type=F32
        )

    @pl.when(step == pl.num_programs(0) - 1)
    def _():
        for group in range(groups):
            found = acc_ref[group].T
            out_ref[group * sub_dim : (group + 1) * sub_dim, :] = (
                found[0:sub_dim] + found[sub_dim : 2 * sub_dim]
            )
            out_ref[groups * sub_dim + group : groups * sub_dim + group + 1, :] = found[
                2 * sub_dim : 2 * sub_dim + 1
            ]


def local_codes(pick, features, codebooks, tables):
    peers = len(tables)
    rows, width = features.shape
    local_k = tables[0].shape[1]
    groups, sub_dim, words = codebooks.shape
    block = block_of(rows, 256)
    depth = 7 * sub_dim
    fixed = lambda shape: pl.BlockSpec(shape, lambda i: (0,) * len(shape))
    return pl.pallas_call(
        functools.partial(codes_kernel, peers=peers),
        grid=(rows // block,),
        out_shape=jax.ShapeDtypeStruct((groups * sub_dim + groups, words), F32),
        in_specs=[
            pl.BlockSpec((2, block), lambda i: (0, i)),
            pl.BlockSpec((block, width), lambda i: (i, 0)),
            fixed(codebooks.shape),
        ]
        + [fixed((width, local_k))] * peers,
        out_specs=fixed((groups * sub_dim + groups, words)),
        scratch_shapes=[
            VMEM((peers * width, local_k), BF16),
            VMEM((groups * words, depth), BF16),
            VMEM((groups, depth, block), BF16),
            VMEM((groups, words, 3 * sub_dim), F32),
        ],
        compiler_params=params(),
        cost_estimate=pl.CostEstimate(
            flops=2 * rows * (peers * width * local_k + groups * words * 256 * 3),
            transcendentals=rows * groups * words,
            bytes_accessed=rows * width * 2 + peers * width * local_k * 2,
        ),
        name="local_codes",
    )(pick, features, codebooks, *tables)


def shards(embeddings, assignment, centroids, codebooks):
    n_sub, n_dp = lax.axis_size("sub"), lax.axis_size("dp")
    sub_at, dp_at = lax.axis_index("sub"), lax.axis_index("dp")
    sub_pos, dp_pos = sub_at[None].astype(jnp.int32), dp_at[None].astype(jnp.int32)
    local_k = centroids.shape[0]
    width = embeddings.shape[1] // n_sub
    groups, sub_dim, words = codebooks.shape

    parts = table_parts(sub_pos, centroids, n_sub)
    tables = [parts[0]] + [swap(parts[hop], "sub", n_sub, hop) for hop in range(1, n_sub)]

    logits, stats = local_logits(centroids, embeddings)
    hop = 1
    while hop < n_sub:
        stats = merge(stats, swap(stats, "sub", n_sub, hop))
        hop *= 2

    found = local_sums(dp_pos, logits, stats, embeddings, n_dp)
    sums, counts = found[:n_dp], found[n_dp:]
    sums = [sums[0]] + [swap(sums[hop], "dp", n_dp, hop) for hop in range(1, n_dp)]
    counts = [counts[0]] + [swap(counts[hop], "dp", n_dp, hop) for hop in range(1, n_dp)]
    mine = update_part(dp_pos, centroids, sums, counts)
    updated = [mine] + [swap(mine, "dp", n_dp, hop) for hop in range(1, n_dp)]
    new_centroids = join_parts(dp_pos, updated)

    pick = jnp.stack([(assignment // local_k) ^ sub_at, assignment % local_k]).astype(jnp.int32)
    features = lax.dynamic_slice_in_dim(embeddings, sub_at * width, width, 1)
    codes = local_codes(pick, features, codebooks, tables)
    pieces = [codes] + [swap(codes, "dp", n_dp, hop) for hop in range(1, n_dp)]
    while len(pieces) > 1:
        pieces = [pieces[i] + pieces[i + 1] for i in range(0, len(pieces), 2)]
    code_sums = pieces[0][: groups * sub_dim].reshape(groups, sub_dim, words)
    code_counts = pieces[0][groups * sub_dim :]
    new_codebooks = (code_sums + codebooks) / (code_counts[:, None, :] + 1.0)
    return (new_centroids, new_codebooks)


def solution(mesh):
    placed = (P("dp", None), P("dp"), P("sub", None), P("sub", None, None))
    return jax.shard_map(
        shards,
        mesh=mesh,
        in_specs=placed,
        out_specs=(P("sub", None), P("sub", None, None)),
        check_vma=False,
    )
```

```python
import functools
import math

import jax
import jax.numpy as jnp
from jax import lax
from jax.experimental import pallas as pl
from jax.experimental.pallas import tpu as pltpu
from jax.sharding import PartitionSpec as P


F32 = jnp.float32
BF16 = jnp.bfloat16
VMEM = pltpu.VMEM
SMEM = pltpu.SMEM
NT = (((1,), (1,)), ((), ()))


def swap(value, axis, size, hop):
    return lax.ppermute(value, axis, [(i, i ^ hop) for i in range(size)])


def block_of(extent, want):
    return want if extent % want == 0 else extent


def params(limit=32 << 20):
    return pltpu.CompilerParams(vmem_limit_bytes=limit)


def encode(value, code_ref):
    scales = []
    for lane in range(0, value.shape[1], 128):
        piece = value[:, lane : lane + 128]
        peak = jnp.maximum(jnp.max(jnp.abs(piece), axis=1, keepdims=True), 1e-30)
        code_ref[:, lane : lane + 128] = jnp.round(piece * (32767.0 / peak)).astype(jnp.int32).astype(jnp.int16)
        scales.append(peak * (1.0 / 32767.0))
    return scales


def decode(code_ref, columns):
    return [
        code_ref[:, lane : lane + 128].astype(jnp.int32).astype(F32)
        * columns[:, lane // 128 : lane // 128 + 1]
        for lane in range(0, code_ref.shape[1], 128)
    ]


def columns_to_rows(columns, count):
    lane = lax.broadcasted_iota(jnp.int32, (columns[0].shape[0], 128), 1)
    wide = jnp.zeros(lane.shape, F32)
    for at, column in enumerate(columns):
        wide = jnp.where(lane == at, column, wide)
    return wide.T[0:count]


def table_kernel(pos_ref, cent_ref, *refs, width):
    outs, flip_ref = refs[:-1], refs[-1]
    flip_ref[...] = cent_ref[...].T
    for hop, out_ref in enumerate(outs):
        start = pl.multiple_of((pos_ref[0] ^ hop) * width, width)
        out_ref[...] = flip_ref[pl.ds(start, width), :]


def table_parts(position, centroids, peers):
    local_k, feat = centroids.shape
    width = feat // peers
    return pl.pallas_call(
        functools.partial(table_kernel, width=width),
        out_shape=[jax.ShapeDtypeStruct((width, local_k), BF16)] * peers,
        in_specs=[pl.BlockSpec(memory_space=SMEM), pl.BlockSpec(memory_space=VMEM)],
        out_specs=[pl.BlockSpec(memory_space=VMEM)] * peers,
        scratch_shapes=[VMEM((feat, local_k), BF16)],
        compiler_params=params(),
        name="table_parts",
    )(position, centroids)


def logits_kernel(cent_ref, rows_ref, logits_ref, stats_ref, half_ref):
    @pl.when(pl.program_id(0) == 0)
    def _():
        wide = cent_ref[...].astype(F32)
        half_ref[...] = jnp.broadcast_to(
            0.5 * jnp.sum(wide * wide, axis=1, keepdims=True), half_ref.shape
        )

    logits = (
        lax.dot_general(cent_ref[...], rows_ref[...], NT, preferred_element_type=F32)
        - half_ref[:, 0:1]
    )
    logits_ref[...] = logits
    peak = jnp.max(logits, axis=0, keepdims=True)
    stats_ref[0:1, :] = peak
    stats_ref[1:2, :] = jnp.sum(jnp.exp(logits - peak), axis=0, keepdims=True)


def local_logits(centroids, embeddings):
    local_k, feat = centroids.shape
    rows = embeddings.shape[0]
    block = block_of(rows, 1024)
    return pl.pallas_call(
        logits_kernel,
        grid=(rows // block,),
        out_shape=[
            jax.ShapeDtypeStruct((local_k, rows), F32),
            jax.ShapeDtypeStruct((2, rows), F32),
        ],
        in_specs=[
            pl.BlockSpec((local_k, feat), lambda i: (0, 0)),
            pl.BlockSpec((block, feat), lambda i: (i, 0)),
        ],
        out_specs=[
            pl.BlockSpec((local_k, block), lambda i: (0, i)),
            pl.BlockSpec((2, block), lambda i: (0, i)),
        ],
        scratch_shapes=[VMEM((local_k, 128), F32)],
        compiler_params=params(),
        cost_estimate=pl.CostEstimate(
            flops=2 * local_k * rows * feat,
            transcendentals=local_k * rows,
            bytes_accessed=rows * feat * 2 + local_k * rows * 4,
        ),
        name="local_logits",
    )(centroids, embeddings)


def merge(former, latter):
    peak = jnp.maximum(former[0:1], latter[0:1])
    total = former[1:2] * jnp.exp(former[0:1] - peak) + latter[1:2] * jnp.exp(latter[0:1] - peak)
    return jnp.concatenate([peak, total], axis=0)


def sums_kernel(pos_ref, logits_ref, stats_ref, rows_ref, *refs, peers):
    own_ref, own_count_ref = refs[:2]
    outs, sides, (acc_ref, count_ref) = refs[2 : peers + 1], refs[peers + 1 : 2 * peers], refs[2 * peers :]
    step = pl.program_id(0)
    probability = jnp.exp(logits_ref[...] - stats_ref[0:1, :]) * (1.0 / stats_ref[1:2, :])
    partial = probability[:, 0:128]
    for lane in range(128, probability.shape[1], 128):
        partial = partial + probability[:, lane : lane + 128]
    sums = jnp.dot(probability.astype(BF16), rows_ref[...], preferred_element_type=F32)

    @pl.when(step == 0)
    def _():
        acc_ref[...] = sums
        count_ref[...] = partial

    @pl.when(step > 0)
    def _():
        acc_ref[...] += sums
        count_ref[...] += partial

    @pl.when(step == pl.num_programs(0) - 1)
    def _():
        part = own_ref.shape[0]
        for hop in range(peers):
            start = pl.multiple_of((pos_ref[0] ^ hop) * part, part)
            count = jnp.sum(count_ref[pl.ds(start, part), :], axis=1, keepdims=True)
            if hop == 0:
                own_ref[...] = acc_ref[pl.ds(start, part), :]
                own_count_ref[...] = jnp.broadcast_to(count, own_count_ref.shape)
            else:
                scales = encode(acc_ref[pl.ds(start, part), :], outs[hop - 1])
                sides[hop - 1][...] = columns_to_rows(scales + [count], 16)


def local_sums(position, logits, stats, embeddings, peers):
    local_k, rows = logits.shape
    feat = embeddings.shape[1]
    block = block_of(rows, 1024)
    part = local_k // peers
    whole = lambda shape: pl.BlockSpec(shape, lambda i: (0, 0))
    return pl.pallas_call(
        functools.partial(sums_kernel, peers=peers),
        grid=(rows // block,),
        out_shape=[jax.ShapeDtypeStruct((part, feat), F32), jax.ShapeDtypeStruct((part, 128), F32)]
        + [jax.ShapeDtypeStruct((part, feat), jnp.int16)] * (peers - 1)
        + [jax.ShapeDtypeStruct((16, part), F32)] * (peers - 1),
        in_specs=[
            pl.BlockSpec(memory_space=SMEM),
            pl.BlockSpec((local_k, block), lambda i: (0, i)),
            pl.BlockSpec((2, block), lambda i: (0, i)),
            pl.BlockSpec((block, feat), lambda i: (i, 0)),
        ],
        out_specs=[whole((part, feat)), whole((part, 128))]
        + [whole((part, feat))] * (peers - 1)
        + [whole((16, part))] * (peers - 1),
        scratch_shapes=[VMEM((local_k, feat), F32), VMEM((local_k, 128), F32)],
        compiler_params=params(),
        cost_estimate=pl.CostEstimate(
            flops=2 * local_k * rows * feat,
            transcendentals=local_k * rows,
            bytes_accessed=rows * feat * 2 + local_k * rows * 4,
        ),
        name="local_sums",
    )(position, logits, stats, embeddings)


def update_kernel(pos_ref, cent_ref, own_ref, own_count_ref, *refs, peers):
    codes, sides, (out_ref, side_ref) = refs[: peers - 1], refs[peers - 1 : 2 * peers - 2], refs[2 * peers - 2 :]
    part, feat = own_ref.shape
    blocks = feat // 128
    columns = [side[...].T for side in sides]
    count = own_count_ref[:, 0:1]
    total = [own_ref[:, lane : lane + 128] for lane in range(0, feat, 128)]
    for code, column in zip(codes, columns):
        count = count + column[:, blocks : blocks + 1]
        total = [former + latter for former, latter in zip(total, decode(code, column))]
    start = pl.multiple_of(pos_ref[0] * part, part)
    cent = cent_ref[pl.ds(start, part), :].astype(F32)
    value = (jnp.concatenate(total, axis=1) + cent) / (count + 1.0)
    side_ref[...] = columns_to_rows(encode(value, out_ref), 16)


def update_part(position, centroids, own, own_count, codes, sides):
    part, feat = own.shape
    return pl.pallas_call(
        functools.partial(update_kernel, peers=len(codes) + 1),
        out_shape=[jax.ShapeDtypeStruct((part, feat), jnp.int16), jax.ShapeDtypeStruct((16, part), F32)],
        in_specs=[pl.BlockSpec(memory_space=SMEM)] + [pl.BlockSpec(memory_space=VMEM)] * (3 + 2 * len(codes)),
        out_specs=[pl.BlockSpec(memory_space=VMEM)] * 2,
        compiler_params=params(16 << 20),
        name="update_part",
    )(position, centroids, own, own_count, *codes, *sides)


def join_kernel(pos_ref, *refs):
    peers = len(refs) // 2
    codes, sides, out_ref = refs[:peers], refs[peers : 2 * peers], refs[-1]
    size = codes[0].shape[0]
    for hop in range(peers):
        start = pl.multiple_of((pos_ref[0] ^ hop) * size, size)
        for at, piece in enumerate(decode(codes[hop], sides[hop][...].T)):
            out_ref[pl.ds(start, size), at * 128 : (at + 1) * 128] = piece


def join_parts(position, codes, sides):
    size, feat = codes[0].shape
    return pl.pallas_call(
        join_kernel,
        out_shape=jax.ShapeDtypeStruct((size * len(codes), feat), F32),
        in_specs=[pl.BlockSpec(memory_space=SMEM)] + [pl.BlockSpec(memory_space=VMEM)] * (2 * len(codes)),
        out_specs=pl.BlockSpec(memory_space=VMEM),
        compiler_params=params(16 << 20),
        name="join_parts",
    )(position, *codes, *sides)


def three_terms(value):
    first = value.astype(BF16)
    rest = value - first.astype(F32)
    second = rest.astype(BF16)
    third = (rest - second.astype(F32)).astype(BF16)
    return first, second, third


def codes_kernel(pick_ref, feats_ref, code_ref, *refs, peers, half):
    refs = refs[:peers] + refs[-5:]
    tables, (out_ref, table_ref, weight_ref, data_ref, acc_ref) = refs[:peers], refs[peers:]
    step = pl.program_id(0)
    groups, sub_dim, words = code_ref.shape
    width, local_k = tables[0].shape
    first_feat = half * width
    block = feats_ref.shape[0]
    depth = data_ref.shape[1]
    head = 3 * sub_dim

    @pl.when(step == 0)
    def _():
        for hop in range(peers):
            table_ref[hop * width : (hop + 1) * width, :] = tables[hop][...]
        scale = 1.0 / math.log(2.0)
        lane_row = lax.broadcasted_iota(jnp.int32, (sub_dim, words), 0)
        for group in range(groups):
            code = code_ref[group]
            first, second, third = three_terms(code * scale)
            half = -0.5 * scale * jnp.sum(code * code, axis=0, keepdims=True)
            bias = [jnp.broadcast_to(t.astype(F32), (sub_dim, words)) for t in three_terms(half)]
            bias = jnp.where(
                lane_row == 0, bias[0], jnp.where(lane_row == 1, bias[1], jnp.where(lane_row == 2, bias[2], 0.0))
            )
            first, second, third = (t.astype(F32) for t in (first, second, third))
            stacked = jnp.concatenate([first, first, bias, second, second, third, third], axis=0)
            weight_ref[group * words : (group + 1) * words, :] = stacked.T.astype(BF16)
        acc_ref[...] = jnp.zeros_like(acc_ref)
        for group in range(groups):
            data_ref[group, 2 * sub_dim : 3 * sub_dim, :] = jnp.ones((sub_dim, block), BF16)

    source, entry = pick_ref[0:1, :], pick_ref[1:2, :]
    hot = (lax.broadcasted_iota(jnp.int32, (local_k, block), 0) == entry).astype(F32).astype(BF16)
    slabs = jnp.dot(table_ref[...], hot, preferred_element_type=F32)
    base = slabs[0:width]
    for hop in range(1, peers):
        base = jnp.where(source == hop, slabs[hop * width : (hop + 1) * width], base)
    minus = (-base).astype(BF16)
    own = feats_ref[...].astype(F32).T.astype(BF16)[first_feat : first_feat + width]
    for group in range(groups):
        span = slice(group * sub_dim, (group + 1) * sub_dim)
        for at in (0, 3, 5):
            data_ref[group, at * sub_dim : (at + 1) * sub_dim, :] = own[span]
            data_ref[group, (at + 1) * sub_dim : (at + 2) * sub_dim, :] = minus[span]
    for group in range(groups):
        logits = jnp.dot(
            weight_ref[group * words : (group + 1) * words, :], data_ref[group], preferred_element_type=F32
        )
        expo = jnp.exp2(logits - jnp.max(logits, axis=0, keepdims=True))
        weights = expo * (1.0 / jnp.sum(expo, axis=0, keepdims=True))
        high = weights.astype(BF16)
        low = (weights - high.astype(F32)).astype(BF16)
        left = data_ref[group, 0:head, :]
        acc_ref[group] += lax.dot_general(high, left, NT, preferred_element_type=F32) + lax.dot_general(
            low, left, NT, preferred_element_type=F32
        )

    @pl.when(step == pl.num_programs(0) - 1)
    def _():
        for group in range(groups):
            found = acc_ref[group].T
            out_ref[group * sub_dim : (group + 1) * sub_dim, :] = (
                found[0:sub_dim] + found[sub_dim : 2 * sub_dim]
            )
            out_ref[groups * sub_dim + group : groups * sub_dim + group + 1, :] = found[
                2 * sub_dim : 2 * sub_dim + 1
            ]


def local_codes(pick, features, codebooks, tables, half, halves, after=()):
    peers = len(tables)
    rows, feats = features.shape
    local_k = tables[0].shape[1]
    groups, sub_dim, words = codebooks.shape
    groups, width = groups // halves, feats // halves
    block = block_of(rows, 1536)
    depth = 7 * sub_dim
    fixed = lambda shape: pl.BlockSpec(shape, lambda i: (0,) * len(shape))
    return pl.pallas_call(
        functools.partial(codes_kernel, peers=peers, half=half),
        grid=(rows // block,),
        out_shape=jax.ShapeDtypeStruct((groups * sub_dim + groups, words), F32),
        in_specs=[
            pl.BlockSpec((2, block), lambda i: (0, i)),
            pl.BlockSpec((block, feats), lambda i: (i, 0)),
            pl.BlockSpec((groups, sub_dim, words), lambda i: (half, 0, 0)),
        ]
        + [pl.BlockSpec((width, local_k), lambda i: (half, 0))] * peers
        + [pl.BlockSpec(memory_space=pl.ANY)] * len(after),
        out_specs=fixed((groups * sub_dim + groups, words)),
        scratch_shapes=[
            VMEM((peers * width, local_k), BF16),
            VMEM((groups * words, depth), BF16),
            VMEM((groups, depth, block), BF16),
            VMEM((groups, words, 3 * sub_dim), F32),
        ],
        compiler_params=params(),
        cost_estimate=pl.CostEstimate(
            flops=2 * rows * (peers * width * local_k + groups * words * 256 * 3),
            transcendentals=rows * groups * words,
            bytes_accessed=rows * width * 2 + peers * width * local_k * 2,
        ),
        name=f"local_codes_{half}",
    )(pick, features, codebooks, *tables, *after)


def shards(embeddings, assignment, centroids, codebooks):
    n_sub, n_dp = lax.axis_size("sub"), lax.axis_size("dp")
    sub_at, dp_at = lax.axis_index("sub"), lax.axis_index("dp")
    sub_pos, dp_pos = sub_at[None].astype(jnp.int32), dp_at[None].astype(jnp.int32)
    local_k = centroids.shape[0]
    width = embeddings.shape[1] // n_sub
    groups, sub_dim, words = codebooks.shape

    parts = table_parts(sub_pos, centroids, n_sub)
    tables = [parts[0]] + [swap(parts[hop], "sub", n_sub, hop) for hop in range(1, n_sub)]

    logits, stats = local_logits(centroids, embeddings)
    hop = 1
    while hop < n_sub:
        stats = merge(stats, swap(stats, "sub", n_sub, hop))
        hop *= 2

    found = local_sums(dp_pos, logits, stats, embeddings, n_dp)
    own, own_count, parts, sides = found[0], found[1], found[2 : n_dp + 1], found[n_dp + 1 :]
    hops = range(1, n_dp)
    parts = [swap(part, "dp", n_dp, hop) for hop, part in zip(hops, parts)]
    sides = [swap(side, "dp", n_dp, hop) for hop, side in zip(hops, sides)]
    code, side = update_part(dp_pos, centroids, own, own_count, parts, sides)
    new_centroids = join_parts(
        dp_pos,
        [code] + [swap(code, "dp", n_dp, hop) for hop in hops],
        [side] + [swap(side, "dp", n_dp, hop) for hop in hops],
    )

    pick = jnp.stack([(assignment // local_k) ^ sub_at, assignment % local_k]).astype(jnp.int32)
    features = lax.dynamic_slice_in_dim(embeddings, sub_at * width, width, 1)
    halves = 2
    found = [
        local_codes(pick, features, codebooks, tables, half, halves, (side,) if half else ())
        for half in range(halves)
    ]
    pieces = [found] + [[swap(each, "dp", n_dp, hop) for each in found] for hop in hops]
    while len(pieces) > 1:
        pieces = [
            [former + latter for former, latter in zip(pieces[i], pieces[i + 1])]
            for i in range(0, len(pieces), 2)
        ]
    each = groups // halves
    code_sums = jnp.concatenate(
        [half[: each * sub_dim].reshape(each, sub_dim, words) for half in pieces[0]], axis=0
    )
    code_counts = jnp.concatenate([half[each * sub_dim :] for half in pieces[0]], axis=0)
    new_codebooks = (code_sums + codebooks) / (code_counts[:, None, :] + 1.0)
    return (new_centroids, new_codebooks)


def solution(mesh):
    placed = (P("dp", None), P("dp"), P("sub", None), P("sub", None, None))
    return jax.shard_map(
        shards,
        mesh=mesh,
        in_specs=placed,
        out_specs=(P("sub", None), P("sub", None, None)),
        check_vma=False,
    )
```

```python
import functools
import math

import jax
import jax.numpy as jnp
from jax import lax
from jax.experimental import pallas as pl
from jax.experimental.pallas import tpu as pltpu
from jax.sharding import PartitionSpec as P


F32 = jnp.float32
BF16 = jnp.bfloat16
VMEM = pltpu.VMEM
SMEM = pltpu.SMEM
NT = (((1,), (1,)), ((), ()))


def swap(value, axis, size, hop):
    return lax.ppermute(value, axis, [(i, i ^ hop) for i in range(size)])


def block_of(extent, want):
    return want if extent % want == 0 else extent


def params(limit=32 << 20):
    return pltpu.CompilerParams(vmem_limit_bytes=limit)


def encode(value, extra, code_ref):
    rows, feat = value.shape
    lane = lax.broadcasted_iota(jnp.int32, (rows, 128), 1)
    tail = jnp.zeros((rows, 128), F32)
    pieces = [value[:, at : at + 128] for at in range(0, feat, 128)]
    if extra is not None:
        pieces.append(extra)
    for at, piece in enumerate(pieces):
        peak = jnp.maximum(jnp.max(jnp.abs(piece), axis=1, keepdims=True), 1e-30)
        exponent = jnp.floor(jnp.log2(peak) * 16.0) + 1.5
        code = jnp.round(piece * (32000.0 * jnp.exp2(exponent * (-1.0 / 16.0))))
        tail = jnp.where(lane == at, exponent - 0.5, tail)
        if at * 128 < feat:
            code_ref[:, at * 128 : (at + 1) * 128] = code.astype(jnp.int32).astype(jnp.int16)
        else:
            tail = jnp.where(lane == 127, code, tail)
    code_ref[:, feat:] = tail.astype(jnp.int32).astype(jnp.int16)


def decode(code_ref):
    feat = code_ref.shape[1] - 128
    tail = code_ref[:, feat:].astype(jnp.int32).astype(F32)
    scale = (1.0 / 32000.0) / jnp.exp2((tail + 0.5) * (-1.0 / 16.0))
    pieces = [
        code_ref[:, at : at + 128].astype(jnp.int32).astype(F32) * scale[:, at // 128 : at // 128 + 1]
        for at in range(0, feat, 128)
    ]
    return pieces, tail[:, 127:128] * scale[:, feat // 128 : feat // 128 + 1]


def table_kernel(pos_ref, cent_ref, *refs, width):
    outs, flip_ref = refs[:-1], refs[-1]
    flip_ref[...] = cent_ref[...].T
    for hop, out_ref in enumerate(outs):
        start = pl.multiple_of((pos_ref[0] ^ hop) * width, width)
        out_ref[...] = flip_ref[pl.ds(start, width), :]


def table_parts(position, centroids, peers):
    local_k, feat = centroids.shape
    width = feat // peers
    return pl.pallas_call(
        functools.partial(table_kernel, width=width),
        out_shape=[jax.ShapeDtypeStruct((width, local_k), BF16)] * peers,
        in_specs=[pl.BlockSpec(memory_space=SMEM), pl.BlockSpec(memory_space=VMEM)],
        out_specs=[pl.BlockSpec(memory_space=VMEM)] * peers,
        scratch_shapes=[VMEM((feat, local_k), BF16)],
        compiler_params=params(),
        name="table_parts",
    )(position, centroids)


def logits_kernel(cent_ref, rows_ref, logits_ref, stats_ref, half_ref):
    @pl.when(pl.program_id(0) == 0)
    def _():
        wide = cent_ref[...].astype(F32)
        half_ref[...] = jnp.broadcast_to(
            0.5 * jnp.sum(wide * wide, axis=1, keepdims=True), half_ref.shape
        )

    logits = (
        lax.dot_general(cent_ref[...], rows_ref[...], NT, preferred_element_type=F32)
        - half_ref[:, 0:1]
    )
    logits_ref[...] = logits
    peak = jnp.max(logits, axis=0, keepdims=True)
    stats_ref[0:1, :] = peak
    stats_ref[1:2, :] = jnp.sum(jnp.exp(logits - peak), axis=0, keepdims=True)


def local_logits(centroids, embeddings):
    local_k, feat = centroids.shape
    rows = embeddings.shape[0]
    block = block_of(rows, 1024)
    return pl.pallas_call(
        logits_kernel,
        grid=(rows // block,),
        out_shape=[
            jax.ShapeDtypeStruct((local_k, rows), F32),
            jax.ShapeDtypeStruct((2, rows), F32),
        ],
        in_specs=[
            pl.BlockSpec((local_k, feat), lambda i: (0, 0)),
            pl.BlockSpec((block, feat), lambda i: (i, 0)),
        ],
        out_specs=[
            pl.BlockSpec((local_k, block), lambda i: (0, i)),
            pl.BlockSpec((2, block), lambda i: (0, i)),
        ],
        scratch_shapes=[VMEM((local_k, 128), F32)],
        compiler_params=params(),
        cost_estimate=pl.CostEstimate(
            flops=2 * local_k * rows * feat,
            transcendentals=local_k * rows,
            bytes_accessed=rows * feat * 2 + local_k * rows * 4,
        ),
        name="local_logits",
    )(centroids, embeddings)


def merge(former, latter):
    peak = jnp.maximum(former[0:1], latter[0:1])
    total = former[1:2] * jnp.exp(former[0:1] - peak) + latter[1:2] * jnp.exp(latter[0:1] - peak)
    return jnp.concatenate([peak, total], axis=0)


def sums_kernel(pos_ref, logits_ref, stats_ref, rows_ref, *refs, peers):
    own_ref, own_count_ref = refs[:2]
    outs, (acc_ref, count_ref) = refs[2 : peers + 1], refs[peers + 1 :]
    step = pl.program_id(0)
    probability = jnp.exp(logits_ref[...] - stats_ref[0:1, :]) * (1.0 / stats_ref[1:2, :])
    partial = probability[:, 0:128]
    for lane in range(128, probability.shape[1], 128):
        partial = partial + probability[:, lane : lane + 128]
    sums = jnp.dot(probability.astype(BF16), rows_ref[...], preferred_element_type=F32)

    @pl.when(step == 0)
    def _():
        acc_ref[...] = sums
        count_ref[...] = partial

    @pl.when(step > 0)
    def _():
        acc_ref[...] += sums
        count_ref[...] += partial

    @pl.when(step == pl.num_programs(0) - 1)
    def _():
        part = own_ref.shape[0]
        for hop in range(peers):
            start = pl.multiple_of((pos_ref[0] ^ hop) * part, part)
            count = jnp.sum(count_ref[pl.ds(start, part), :], axis=1, keepdims=True)
            if hop == 0:
                own_ref[...] = acc_ref[pl.ds(start, part), :]
                own_count_ref[...] = jnp.broadcast_to(count, own_count_ref.shape)
            else:
                encode(acc_ref[pl.ds(start, part), :], count, outs[hop - 1])


def local_sums(position, logits, stats, embeddings, peers):
    local_k, rows = logits.shape
    feat = embeddings.shape[1]
    block = block_of(rows, 1024)
    part = local_k // peers
    whole = lambda shape: pl.BlockSpec(shape, lambda i: (0, 0))
    return pl.pallas_call(
        functools.partial(sums_kernel, peers=peers),
        grid=(rows // block,),
        out_shape=[jax.ShapeDtypeStruct((part, feat), F32), jax.ShapeDtypeStruct((part, 128), F32)]
        + [jax.ShapeDtypeStruct((part, feat + 128), jnp.int16)] * (peers - 1),
        in_specs=[
            pl.BlockSpec(memory_space=SMEM),
            pl.BlockSpec((local_k, block), lambda i: (0, i)),
            pl.BlockSpec((2, block), lambda i: (0, i)),
            pl.BlockSpec((block, feat), lambda i: (i, 0)),
        ],
        out_specs=[whole((part, feat)), whole((part, 128))]
        + [whole((part, feat + 128))] * (peers - 1),
        scratch_shapes=[VMEM((local_k, feat), F32), VMEM((local_k, 128), F32)],
        compiler_params=params(),
        cost_estimate=pl.CostEstimate(
            flops=2 * local_k * rows * feat,
            transcendentals=local_k * rows,
            bytes_accessed=rows * feat * 2 + local_k * rows * 4,
        ),
        name="local_sums",
    )(position, logits, stats, embeddings)


def update_kernel(pos_ref, cent_ref, own_ref, own_count_ref, *refs):
    codes, out_ref = refs[:-1], refs[-1]
    part, feat = own_ref.shape
    count = own_count_ref[:, 0:1]
    total = [own_ref[:, lane : lane + 128] for lane in range(0, feat, 128)]
    for code in codes:
        pieces, more = decode(code)
        count = count + more
        total = [former + latter for former, latter in zip(total, pieces)]
    start = pl.multiple_of(pos_ref[0] * part, part)
    cent = cent_ref[pl.ds(start, part), :].astype(F32)
    encode((jnp.concatenate(total, axis=1) + cent) / (count + 1.0), None, out_ref)


def update_part(position, centroids, own, own_count, codes):
    return pl.pallas_call(
        update_kernel,
        out_shape=jax.ShapeDtypeStruct(codes[0].shape, jnp.int16),
        in_specs=[pl.BlockSpec(memory_space=SMEM)] + [pl.BlockSpec(memory_space=VMEM)] * (3 + len(codes)),
        out_specs=pl.BlockSpec(memory_space=VMEM),
        compiler_params=params(16 << 20),
        name="update_part",
    )(position, centroids, own, own_count, *codes)


def join_kernel(pos_ref, *refs):
    codes, out_ref = refs[:-1], refs[-1]
    size = codes[0].shape[0]
    for hop, code in enumerate(codes):
        start = pl.multiple_of((pos_ref[0] ^ hop) * size, size)
        for at, piece in enumerate(decode(code)[0]):
            out_ref[pl.ds(start, size), at * 128 : (at + 1) * 128] = piece


def join_parts(position, codes):
    size, feat = codes[0].shape
    return pl.pallas_call(
        join_kernel,
        out_shape=jax.ShapeDtypeStruct((size * len(codes), feat - 128), F32),
        in_specs=[pl.BlockSpec(memory_space=SMEM)] + [pl.BlockSpec(memory_space=VMEM)] * len(codes),
        out_specs=pl.BlockSpec(memory_space=VMEM),
        compiler_params=params(16 << 20),
        name="join_parts",
    )(position, *codes)


def three_terms(value):
    first = value.astype(BF16)
    rest = value - first.astype(F32)
    second = rest.astype(BF16)
    third = (rest - second.astype(F32)).astype(BF16)
    return first, second, third


def codes_kernel(pick_ref, feats_ref, code_ref, *refs, peers, half):
    former = refs[peers : peers + 1]
    refs = refs[:peers] + refs[-5:]
    tables, (out_ref, table_ref, weight_ref, data_ref, acc_ref) = refs[:peers], refs[peers:]
    step = pl.program_id(0)
    groups, sub_dim, words = code_ref.shape
    width, local_k = tables[0].shape
    first_feat = half * width
    block = feats_ref.shape[0]
    head = 3 * sub_dim

    @pl.when(step == 0)
    def _():
        for hop in range(peers):
            table_ref[hop * width : (hop + 1) * width, :] = tables[hop][...]
        scale = 1.0 / math.log(2.0)
        lane_row = lax.broadcasted_iota(jnp.int32, (sub_dim, words), 0)
        for group in range(groups):
            code = code_ref[group]
            first, second, third = three_terms(code * scale)
            half = -0.5 * scale * jnp.sum(code * code, axis=0, keepdims=True)
            bias = [jnp.broadcast_to(t.astype(F32), (sub_dim, words)) for t in three_terms(half)]
            bias = jnp.where(
                lane_row == 0, bias[0], jnp.where(lane_row == 1, bias[1], jnp.where(lane_row == 2, bias[2], 0.0))
            )
            first, second, third = (t.astype(F32) for t in (first, second, third))
            stacked = jnp.concatenate([first, first, bias, second, second, third, third], axis=0)
            weight_ref[group * words : (group + 1) * words, :] = stacked.T.astype(BF16)
        acc_ref[...] = jnp.zeros_like(acc_ref)
        for group in range(groups):
            data_ref[group, 2 * sub_dim : 3 * sub_dim, :] = jnp.ones((sub_dim, block), BF16)

    source, entry = pick_ref[0:1, :], pick_ref[1:2, :]
    hot = (lax.broadcasted_iota(jnp.int32, (local_k, block), 0) == entry).astype(F32).astype(BF16)
    slabs = jnp.dot(table_ref[...], hot, preferred_element_type=F32)
    base = slabs[0:width]
    for hop in range(1, peers):
        base = jnp.where(source == hop, slabs[hop * width : (hop + 1) * width], base)
    minus = (-base).astype(BF16)
    own = feats_ref[...].astype(F32).T.astype(BF16)[first_feat : first_feat + width]
    for group in range(groups):
        span = slice(group * sub_dim, (group + 1) * sub_dim)
        for at in (0, 3, 5):
            data_ref[group, at * sub_dim : (at + 1) * sub_dim, :] = own[span]
            data_ref[group, (at + 1) * sub_dim : (at + 2) * sub_dim, :] = minus[span]
    for group in range(groups):
        logits = jnp.dot(
            weight_ref[group * words : (group + 1) * words, :], data_ref[group], preferred_element_type=F32
        )
        expo = jnp.exp2(logits - jnp.max(logits, axis=0, keepdims=True))
        weights = expo * (1.0 / jnp.sum(expo, axis=0, keepdims=True))
        high = weights.astype(BF16)
        low = (weights - high.astype(F32)).astype(BF16)
        left = data_ref[group, 0:head, :]
        acc_ref[group] += lax.dot_general(high, left, NT, preferred_element_type=F32) + lax.dot_general(
            low, left, NT, preferred_element_type=F32
        )

    @pl.when(step == pl.num_programs(0) - 1)
    def _():
        if half:
            out_ref[0 : former[0].shape[0], :] = former[0][...]
        first_row, first_count = half * groups * sub_dim, out_ref.shape[0] - (half + 1) * groups
        if half:
            out_ref[first_count + groups :, :] = former[0][half * groups * sub_dim :, :]
        for group in range(groups):
            found = acc_ref[group].T
            row = first_row + group * sub_dim
            out_ref[row : row + sub_dim, :] = found[0:sub_dim] + found[sub_dim : 2 * sub_dim]
            out_ref[first_count + group : first_count + group + 1, :] = found[2 * sub_dim : 2 * sub_dim + 1]


def local_codes(pick, features, codebooks, tables, half, halves, former=(), after=()):
    peers = len(tables)
    rows, feats = features.shape
    local_k = tables[0].shape[1]
    groups, sub_dim, words = codebooks.shape
    groups, width = groups // halves, feats // halves
    block = block_of(rows, 1536)
    depth = 7 * sub_dim
    fixed = lambda shape: pl.BlockSpec(shape, lambda i: (0,) * len(shape))
    return pl.pallas_call(
        functools.partial(codes_kernel, peers=peers, half=half),
        grid=(rows // block,),
        out_shape=jax.ShapeDtypeStruct(((half + 1) * groups * (sub_dim + 1), words), F32),
        in_specs=[
            pl.BlockSpec((2, block), lambda i: (0, i)),
            pl.BlockSpec((block, feats), lambda i: (i, 0)),
            pl.BlockSpec((groups, sub_dim, words), lambda i: (half, 0, 0)),
        ]
        + [pl.BlockSpec((width, local_k), lambda i: (half, 0))] * peers
        + [fixed(each.shape) for each in former]
        + [pl.BlockSpec(memory_space=pl.ANY)] * len(after),
        out_specs=fixed(((half + 1) * groups * (sub_dim + 1), words)),
        scratch_shapes=[
            VMEM((peers * width, local_k), BF16),
            VMEM((groups * words, depth), BF16),
            VMEM((groups, depth, block), BF16),
            VMEM((groups, words, 3 * sub_dim), F32),
        ],
        compiler_params=params(),
        cost_estimate=pl.CostEstimate(
            flops=2 * rows * (peers * width * local_k + groups * words * 256 * 3),
            transcendentals=rows * groups * words,
            bytes_accessed=rows * width * 2 + peers * width * local_k * 2,
        ),
    )(pick, features, codebooks, *tables, *former, *after)


def after(value, *others):
    return lax.optimization_barrier((value, *others))[0]


def shards(embeddings, assignment, centroids, codebooks):
    n_sub, n_dp = lax.axis_size("sub"), lax.axis_size("dp")
    sub_at, dp_at = lax.axis_index("sub"), lax.axis_index("dp")
    sub_pos, dp_pos = sub_at[None].astype(jnp.int32), dp_at[None].astype(jnp.int32)
    local_k = centroids.shape[0]
    width = embeddings.shape[1] // n_sub
    groups, sub_dim, words = codebooks.shape
    hops = range(1, n_dp)

    parts = table_parts(sub_pos, centroids, n_sub)
    tables = [parts[0]] + [None] * (n_sub - 1)

    def send_table(hop, *others):
        tables[hop] = swap(after(parts[hop], *others), "sub", n_sub, hop)

    for hop in EARLY:
        send_table(hop)
    logits, stats = local_logits(centroids, embeddings)
    hop = 1
    while hop < n_sub:
        other = swap(stats, "sub", n_sub, hop)
        stats = merge(stats, other)
        hop *= 2
    for hop in range(n_sub - 1, 0, -1):
        if tables[hop] is None:
            send_table(hop, stats)

    found = local_sums(dp_pos, logits, stats, embeddings, n_dp)
    own, own_count, sums = found[0], found[1], list(found[2:])
    for hop in hops:
        sums[hop - 1] = swap(sums[hop - 1], "dp", n_dp, hop)
    code = update_part(dp_pos, centroids, own, own_count, sums)
    updated = [code]
    for hop in hops:
        updated.append(swap(code, "dp", n_dp, hop))
    new_centroids = join_parts(dp_pos, updated)

    pick = jnp.stack([(assignment // local_k) ^ sub_at, assignment % local_k]).astype(jnp.int32)
    features = lax.dynamic_slice_in_dim(embeddings, sub_at * width, width, 1)
    found = local_codes(pick, features, codebooks, tables, 0, 2)
    found = local_codes(pick, features, codebooks, tables, 1, 2, (found,), (code,))
    pieces = [found]
    for hop in hops:
        pieces.append(swap(found, "dp", n_dp, hop))
    while len(pieces) > 1:
        pieces = [pieces[i] + pieces[i + 1] for i in range(0, len(pieces), 2)]
    total, each = pieces[0], groups // 2
    code_sums = total[: groups * sub_dim].reshape(groups, sub_dim, words)
    code_counts = jnp.concatenate([total[groups * sub_dim + each :], total[groups * sub_dim : groups * sub_dim + each]])
    new_codebooks = (code_sums + codebooks) / (code_counts[:, None, :] + 1.0)
    return (new_centroids, new_codebooks)


EARLY = (6, 7, 2, 3)


def solution(mesh):
    placed = (P("dp", None), P("dp"), P("sub", None), P("sub", None, None))
    return jax.shard_map(
        shards,
        mesh=mesh,
        in_specs=placed,
        out_specs=(P("sub", None), P("sub", None, None)),
        check_vma=False,
    )
```

```python
import functools
import math

import jax
import jax.numpy as jnp
from jax import lax
from jax.experimental import pallas as pl
from jax.experimental.pallas import tpu as pltpu
from jax.sharding import PartitionSpec as P


F32 = jnp.float32
BF16 = jnp.bfloat16
VMEM = pltpu.VMEM
SMEM = pltpu.SMEM
NT = (((1,), (1,)), ((), ()))


def swap(value, axis, size, hop):
    return lax.ppermute(value, axis, [(i, i ^ hop) for i in range(size)])


def block_of(extent, want):
    return want if extent % want == 0 else extent


def params(limit=32 << 20):
    return pltpu.CompilerParams(vmem_limit_bytes=limit)


def encode(value, extra, code_ref):
    rows, feat = value.shape
    lane = lax.broadcasted_iota(jnp.int32, (rows, 128), 1)
    tail = jnp.zeros((rows, 128), F32)
    pieces = [value[:, at : at + 128] for at in range(0, feat, 128)]
    if extra is not None:
        pieces.append(extra)
    for at, piece in enumerate(pieces):
        peak = jnp.maximum(jnp.max(jnp.abs(piece), axis=1, keepdims=True), 1e-30)
        exponent = jnp.floor(jnp.log2(peak) * 16.0) + 1.5
        code = jnp.round(piece * (32000.0 * jnp.exp2(exponent * (-1.0 / 16.0))))
        tail = jnp.where(lane == at, exponent - 0.5, tail)
        if at * 128 < feat:
            code_ref[:, at * 128 : (at + 1) * 128] = code.astype(jnp.int32).astype(jnp.int16)
        else:
            tail = jnp.where(lane == 127, code, tail)
    code_ref[:, feat:] = tail.astype(jnp.int32).astype(jnp.int16)


def decode(code_ref):
    feat = code_ref.shape[1] - 128
    tail = code_ref[:, feat:].astype(jnp.int32).astype(F32)
    scale = (1.0 / 32000.0) / jnp.exp2((tail + 0.5) * (-1.0 / 16.0))
    pieces = [
        code_ref[:, at : at + 128].astype(jnp.int32).astype(F32) * scale[:, at // 128 : at // 128 + 1]
        for at in range(0, feat, 128)
    ]
    return pieces, tail[:, 127:128] * scale[:, feat // 128 : feat // 128 + 1]


def table_kernel(pos_ref, cent_ref, *refs, width):
    outs, flip_ref = refs[:-1], refs[-1]
    flip_ref[...] = cent_ref[...].T
    for hop, out_ref in enumerate(outs):
        start = pl.multiple_of((pos_ref[0] ^ hop) * width, width)
        out_ref[...] = flip_ref[pl.ds(start, width), :]


def table_parts(position, centroids, peers):
    local_k, feat = centroids.shape
    width = feat // peers
    return pl.pallas_call(
        functools.partial(table_kernel, width=width),
        out_shape=[jax.ShapeDtypeStruct((width, local_k), BF16)] * peers,
        in_specs=[pl.BlockSpec(memory_space=SMEM), pl.BlockSpec(memory_space=VMEM)],
        out_specs=[pl.BlockSpec(memory_space=VMEM)] * peers,
        scratch_shapes=[VMEM((feat, local_k), BF16)],
        compiler_params=params(),
        name="table_parts",
    )(position, centroids)


def spans(rows):
    short = block_of(rows, 512)
    cuts = [0, short] if rows > short else [0]
    while rows - cuts[-1] > 2 * short:
        cuts.append(cuts[-1] + 2 * short)
    if rows - cuts[-1] > short:
        cuts.append(cuts[-1] + short)
    return list(zip(cuts, cuts[1:] + [rows]))


def logits_kernel(cent_hbm, rows_hbm, logits_hbm, stats_ref, cent_ref, rows_ref, logits_ref, in_sem, out_sem):
    parts = spans(rows_hbm.shape[0])
    copies = [pltpu.make_async_copy(cent_hbm, cent_ref, in_sem.at[len(parts)])]
    copies += [
        pltpu.make_async_copy(rows_hbm.at[lo:hi], rows_ref.at[lo:hi], in_sem.at[at])
        for at, (lo, hi) in enumerate(parts)
    ]
    for copy in copies:
        copy.start()
    copies[0].wait()
    wide = cent_ref[...].astype(F32)
    half = 0.5 * jnp.sum(wide * wide, axis=1, keepdims=True)
    outs = []
    for at, (lo, hi) in enumerate(parts):
        copies[1 + at].wait()
        logits = (
            lax.dot_general(cent_ref[...], rows_ref[lo:hi, :], NT, preferred_element_type=F32) - half
        )
        logits_ref[:, lo:hi] = logits
        outs.append(pltpu.make_async_copy(logits_ref.at[:, lo:hi], logits_hbm.at[:, lo:hi], out_sem.at[at]))
        outs[-1].start()
        peak = jnp.max(logits, axis=0, keepdims=True)
        stats_ref[0:1, lo:hi] = peak
        stats_ref[1:2, lo:hi] = jnp.sum(jnp.exp(logits - peak), axis=0, keepdims=True)
    for out in outs:
        out.wait()


def local_logits(centroids, embeddings):
    local_k, feat = centroids.shape
    rows = embeddings.shape[0]
    parts = len(spans(rows))
    return pl.pallas_call(
        logits_kernel,
        out_shape=[
            jax.ShapeDtypeStruct((local_k, rows), F32),
            jax.ShapeDtypeStruct((2, rows), F32),
        ],
        in_specs=[pl.BlockSpec(memory_space=pltpu.HBM)] * 2,
        out_specs=[pl.BlockSpec(memory_space=pltpu.HBM), pl.BlockSpec(memory_space=VMEM)],
        scratch_shapes=[
            VMEM((local_k, feat), BF16),
            VMEM((rows, feat), BF16),
            VMEM((local_k, rows), F32),
            pltpu.SemaphoreType.DMA((parts + 1,)),
            pltpu.SemaphoreType.DMA((parts,)),
        ],
        compiler_params=params(54 << 20),
        cost_estimate=pl.CostEstimate(
            flops=2 * local_k * rows * feat,
            transcendentals=local_k * rows,
            bytes_accessed=rows * feat * 2 + local_k * rows * 4,
        ),
        name="local_logits",
    )(centroids, embeddings)


def merge(former, latter):
    peak = jnp.maximum(former[0:1], latter[0:1])
    total = former[1:2] * jnp.exp(former[0:1] - peak) + latter[1:2] * jnp.exp(latter[0:1] - peak)
    return jnp.concatenate([peak, total], axis=0)


def sums_kernel(pos_ref, logits_hbm, stats_ref, rows_hbm, own_ref, own_count_ref, *refs, peers):
    outs, (acc_ref, rows_ref, logits_ref, sem) = refs[: peers - 1], refs[peers - 1 :]
    parts = spans(rows_hbm.shape[0])
    copies = [
        (
            pltpu.make_async_copy(logits_hbm.at[:, lo:hi], logits_ref.at[:, lo:hi], sem.at[0, at]),
            pltpu.make_async_copy(rows_hbm.at[lo:hi], rows_ref.at[lo:hi], sem.at[1, at]),
        )
        for at, (lo, hi) in enumerate(parts)
    ]
    for pair in copies:
        for copy in pair:
            copy.start()
    count = None
    for (lo, hi), pair in zip(parts, copies):
        for copy in pair:
            copy.wait()
        probability = jnp.exp(logits_ref[:, lo:hi] - stats_ref[0:1, lo:hi]) * (1.0 / stats_ref[1:2, lo:hi])
        for lane in range(0, hi - lo, 128):
            piece = probability[:, lane : lane + 128]
            count = piece if count is None else count + piece
        sums = jnp.dot(probability.astype(BF16), rows_ref[lo:hi, :], preferred_element_type=F32)
        if lo == 0:
            acc_ref[...] = sums
        else:
            acc_ref[...] += sums
    part = own_ref.shape[0]
    logits_ref[:, 0:128] = jnp.broadcast_to(jnp.sum(count, axis=1, keepdims=True), count.shape)
    for hop in range(peers):
        start = pl.multiple_of((pos_ref[0] ^ hop) * part, part)
        total, weight = acc_ref[pl.ds(start, part), :], logits_ref[pl.ds(start, part), 0:128]
        if hop == 0:
            own_ref[...] = total
            own_count_ref[...] = weight
        else:
            encode(total, weight, outs[hop - 1])


def local_sums(position, logits, stats, embeddings, peers):
    local_k, rows = logits.shape
    feat = embeddings.shape[1]
    part = local_k // peers
    in_vmem, in_hbm = pl.BlockSpec(memory_space=VMEM), pl.BlockSpec(memory_space=pltpu.HBM)
    return pl.pallas_call(
        functools.partial(sums_kernel, peers=peers),
        out_shape=[jax.ShapeDtypeStruct((part, feat), F32), jax.ShapeDtypeStruct((part, 128), F32)]
        + [jax.ShapeDtypeStruct((part, feat + 128), jnp.int16)] * (peers - 1),
        in_specs=[pl.BlockSpec(memory_space=SMEM), in_hbm, in_vmem, in_hbm],
        out_specs=[in_vmem] * (peers + 1),
        scratch_shapes=[
            VMEM((local_k, feat), F32),
            VMEM((rows, feat), BF16),
            VMEM((local_k, rows), F32),
            pltpu.SemaphoreType.DMA((2, len(spans(rows)))),
        ],
        compiler_params=params(50 << 20),
        cost_estimate=pl.CostEstimate(
            flops=2 * local_k * rows * feat,
            transcendentals=local_k * rows,
            bytes_accessed=rows * feat * 2 + local_k * rows * 4,
        ),
        name="local_sums",
    )(position, logits, stats, embeddings)


def update_kernel(pos_ref, cent_ref, own_ref, own_count_ref, *refs):
    codes, out_ref = refs[:-1], refs[-1]
    part, feat = own_ref.shape
    count = own_count_ref[:, 0:1]
    total = [own_ref[:, lane : lane + 128] for lane in range(0, feat, 128)]
    for code in codes:
        pieces, more = decode(code)
        count = count + more
        total = [former + latter for former, latter in zip(total, pieces)]
    start = pl.multiple_of(pos_ref[0] * part, part)
    cent = cent_ref[pl.ds(start, part), :].astype(F32)
    encode((jnp.concatenate(total, axis=1) + cent) / (count + 1.0), None, out_ref)


def update_part(position, centroids, own, own_count, codes):
    return pl.pallas_call(
        update_kernel,
        out_shape=jax.ShapeDtypeStruct(codes[0].shape, jnp.int16),
        in_specs=[pl.BlockSpec(memory_space=SMEM)] + [pl.BlockSpec(memory_space=VMEM)] * (3 + len(codes)),
        out_specs=pl.BlockSpec(memory_space=VMEM),
        compiler_params=params(16 << 20),
        name="update_part",
    )(position, centroids, own, own_count, *codes)


def join_kernel(pos_ref, *refs):
    codes, out_ref = refs[:-1], refs[-1]
    size = codes[0].shape[0]
    for hop, code in enumerate(codes):
        start = pl.multiple_of((pos_ref[0] ^ hop) * size, size)
        for at, piece in enumerate(decode(code)[0]):
            out_ref[pl.ds(start, size), at * 128 : (at + 1) * 128] = piece


def join_parts(position, codes):
    size, feat = codes[0].shape
    return pl.pallas_call(
        join_kernel,
        out_shape=jax.ShapeDtypeStruct((size * len(codes), feat - 128), F32),
        in_specs=[pl.BlockSpec(memory_space=SMEM)] + [pl.BlockSpec(memory_space=VMEM)] * len(codes),
        out_specs=pl.BlockSpec(memory_space=VMEM),
        compiler_params=params(16 << 20),
        name="join_parts",
    )(position, *codes)


def three_terms(value):
    first = value.astype(BF16)
    rest = value - first.astype(F32)
    second = rest.astype(BF16)
    third = (rest - second.astype(F32)).astype(BF16)
    return first, second, third


def codes_kernel(pick_ref, feats_ref, code_ref, *refs, peers, first, last):
    former = refs[peers : peers + 1]
    refs = refs[:peers] + refs[-5:]
    tables, (out_ref, table_ref, weight_ref, data_ref, acc_ref) = refs[:peers], refs[peers:]
    step = pl.program_id(0)
    groups, sub_dim, words = last - first, *code_ref.shape[1:]
    width, local_k = groups * sub_dim, tables[0].shape[1]
    first_feat = first * sub_dim
    block = feats_ref.shape[0]
    head = 3 * sub_dim

    @pl.when(step == 0)
    def _():
        for hop in range(peers):
            table_ref[hop * width : (hop + 1) * width, :] = tables[hop][first_feat : first_feat + width, :]
        scale = 1.0 / math.log(2.0)
        lane_row = lax.broadcasted_iota(jnp.int32, (sub_dim, words), 0)
        for group in range(groups):
            code = code_ref[first + group]
            one, two, three = three_terms(code * scale)
            half = -0.5 * scale * jnp.sum(code * code, axis=0, keepdims=True)
            bias = [jnp.broadcast_to(t.astype(F32), (sub_dim, words)) for t in three_terms(half)]
            bias = jnp.where(
                lane_row == 0, bias[0], jnp.where(lane_row == 1, bias[1], jnp.where(lane_row == 2, bias[2], 0.0))
            )
            one, two, three = (t.astype(F32) for t in (one, two, three))
            stacked = jnp.concatenate([one, one, bias, two, two, three, three], axis=0)
            weight_ref[group * words : (group + 1) * words, :] = stacked.T.astype(BF16)
        acc_ref[...] = jnp.zeros_like(acc_ref)
        for group in range(groups):
            data_ref[group, 2 * sub_dim : 3 * sub_dim, :] = jnp.ones((sub_dim, block), BF16)

    source, entry = pick_ref[0:1, :], pick_ref[1:2, :]
    hot = (lax.broadcasted_iota(jnp.int32, (local_k, block), 0) == entry).astype(F32).astype(BF16)
    slabs = jnp.dot(table_ref[...], hot, preferred_element_type=F32)
    base = slabs[0:width]
    for hop in range(1, peers):
        base = jnp.where(source == hop, slabs[hop * width : (hop + 1) * width], base)
    minus = (-base).astype(BF16)
    own = feats_ref[...].astype(F32).T.astype(BF16)[first_feat : first_feat + width]
    for group in range(groups):
        span = slice(group * sub_dim, (group + 1) * sub_dim)
        for at in (0, 3, 5):
            data_ref[group, at * sub_dim : (at + 1) * sub_dim, :] = own[span]
            data_ref[group, (at + 1) * sub_dim : (at + 2) * sub_dim, :] = minus[span]
    for group in range(groups):
        logits = jnp.dot(
            weight_ref[group * words : (group + 1) * words, :], data_ref[group], preferred_element_type=F32
        )
        expo = jnp.exp2(logits - jnp.max(logits, axis=0, keepdims=True))
        weights = expo * (1.0 / jnp.sum(expo, axis=0, keepdims=True))
        high = weights.astype(BF16)
        low = (weights - high.astype(F32)).astype(BF16)
        left = data_ref[group, 0:head, :]
        acc_ref[group] += lax.dot_general(high, left, NT, preferred_element_type=F32) + lax.dot_general(
            low, left, NT, preferred_element_type=F32
        )

    @pl.when(step == pl.num_programs(0) - 1)
    def _():
        counts = last * sub_dim
        if first:
            out_ref[0:first_feat, :] = former[0][0:first_feat, :]
            out_ref[counts : counts + first, :] = former[0][first_feat:, :]
        for group in range(groups):
            found = acc_ref[group].T
            row = first_feat + group * sub_dim
            out_ref[row : row + sub_dim, :] = found[0:sub_dim] + found[sub_dim : 2 * sub_dim]
            out_ref[counts + first + group : counts + first + group + 1, :] = found[
                2 * sub_dim : 2 * sub_dim + 1
            ]


def local_codes(pick, features, codebooks, tables, first, last, former=(), after=()):
    peers = len(tables)
    rows, feats = features.shape
    local_k = tables[0].shape[1]
    sub_dim, words = codebooks.shape[1:]
    groups = last - first
    width = groups * sub_dim
    block = block_of(rows, 1536)
    depth = 7 * sub_dim
    fixed = lambda shape: pl.BlockSpec(shape, lambda i: (0,) * len(shape))
    return pl.pallas_call(
        functools.partial(codes_kernel, peers=peers, first=first, last=last),
        grid=(rows // block,),
        out_shape=jax.ShapeDtypeStruct((last * (sub_dim + 1), words), F32),
        in_specs=[
            pl.BlockSpec((2, block), lambda i: (0, i)),
            pl.BlockSpec((block, feats), lambda i: (i, 0)),
            fixed(codebooks.shape),
        ]
        + [fixed((feats, local_k))] * peers
        + [fixed(each.shape) for each in former]
        + [pl.BlockSpec(memory_space=pl.ANY)] * len(after),
        out_specs=fixed((last * (sub_dim + 1), words)),
        scratch_shapes=[
            VMEM((peers * width, local_k), BF16),
            VMEM((groups * words, depth), BF16),
            VMEM((groups, depth, block), BF16),
            VMEM((groups, words, 3 * sub_dim), F32),
        ],
        compiler_params=params(),
        cost_estimate=pl.CostEstimate(
            flops=2 * rows * (peers * width * local_k + groups * words * 256 * 3),
            transcendentals=rows * groups * words,
            bytes_accessed=rows * width * 2 + peers * width * local_k * 2,
        ),
        name="local_codes",
    )(pick, features, codebooks, *tables, *former, *after)


def after(value, *others):
    return lax.optimization_barrier((value, *others))[0]


def shards(embeddings, assignment, centroids, codebooks):
    n_sub, n_dp = lax.axis_size("sub"), lax.axis_size("dp")
    sub_at, dp_at = lax.axis_index("sub"), lax.axis_index("dp")
    sub_pos, dp_pos = sub_at[None].astype(jnp.int32), dp_at[None].astype(jnp.int32)
    local_k = centroids.shape[0]
    width = embeddings.shape[1] // n_sub
    groups, sub_dim, words = codebooks.shape
    hops = range(1, n_dp)

    parts = table_parts(sub_pos, centroids, n_sub)
    tables = [parts[0]] + [None] * (n_sub - 1)

    def send_table(hop, *others):
        tables[hop] = swap(after(parts[hop], *others), "sub", n_sub, hop)

    for hop in EARLY:
        send_table(hop)
    logits, stats = local_logits(centroids, embeddings)
    hop = 1
    while hop < n_sub:
        other = swap(stats, "sub", n_sub, hop)
        stats = merge(stats, other)
        hop *= 2
    for hop in range(n_sub - 1, 0, -1):
        if tables[hop] is None:
            send_table(hop, stats)

    found = local_sums(dp_pos, logits, stats, embeddings, n_dp)
    own, own_count, sums = found[0], found[1], list(found[2:])
    for hop in hops:
        sums[hop - 1] = swap(sums[hop - 1], "dp", n_dp, hop)
    code = update_part(dp_pos, centroids, own, own_count, sums)
    updated = [code]
    for hop in hops:
        updated.append(swap(code, "dp", n_dp, hop))
    new_centroids = join_parts(dp_pos, updated)

    pick = jnp.stack([(assignment // local_k) ^ sub_at, assignment % local_k]).astype(jnp.int32)
    features = lax.dynamic_slice_in_dim(embeddings, sub_at * width, width, 1)
    early = (groups * 5 + 7) // 8
    found = local_codes(pick, features, codebooks, tables, 0, early)
    found = local_codes(pick, features, codebooks, tables, early, groups, (found,), (code,))
    pieces = [found]
    for hop in hops:
        pieces.append(swap(found, "dp", n_dp, hop))
    while len(pieces) > 1:
        pieces = [pieces[i] + pieces[i + 1] for i in range(0, len(pieces), 2)]
    code_sums = pieces[0][: groups * sub_dim].reshape(groups, sub_dim, words)
    code_counts = pieces[0][groups * sub_dim :]
    new_codebooks = (code_sums + codebooks) / (code_counts[:, None, :] + 1.0)
    return (new_centroids, new_codebooks)


EARLY = (6, 7, 2, 3)


def solution(mesh):
    placed = (P("dp", None), P("dp"), P("sub", None), P("sub", None, None))
    return jax.shard_map(
        shards,
        mesh=mesh,
        in_specs=placed,
        out_specs=(P("sub", None), P("sub", None, None)),
        check_vma=False,
    )
```
